32 devices in a mesh: subset: 8 (over z, x), vocab: 4 (over y, core).
Axes of the slice: x: 2, y: 2, z: 4, core: 2. Of those that a mesh axis runs over, the one named last changes fastest.
Arguments:
- hidden: bfloat16 [4096, 2048], P('subset', 'vocab'), may hold values from -100 to 100
- proj_weight: bfloat16 [2048, 25600], P('subset', 'vocab'), may hold values from -1 to 1
- targets: int32 [4096], P('subset'), may hold values from 0 to 25599
- counts: int32 [8, 100, 512], P('subset', 'vocab'), may hold values from 1 to 15, as said below
- ranks: int32 [8], replicated, may hold values from 0 to 799
Outputs:
- row_cross_entropy: float32 [4096], P('subset')
- resample_mean_losses: float32 [8, 100], P('subset', 'vocab')
- quantiles: float32 [8], replicated
The draws below stay inside these ranges and needn't reach their ends.
Inputs may be any that keep to these rules, and one draw needn't show every extreme that they name: For every subset and resample the counts over the 512 rows sum to 4096.
All inputs are finite; a program needn't handle non-finite values.
Results may differ from the reference program's by a relative error of at most 0.0003.
Values may be sent and summed in bfloat16 or wider, within the bound.
No kernel may reach another device: no remote copies, remote signals or barrier semaphores. Data moves between devices by JAX's collectives and lax.ppermute only.
A program may use at most 128 MiB of HBM per device.

```python
import jax
import jax.numpy as jnp
from jax import lax

D = 2048
ROWS = 512
RESAMPLES = 100
QUANT = 8
VOCAB = 25600
SUBSETS = 8
TOKEN_ROW_COUNT = 4096


def shared_weight(key):
    values = jax.random.normal(jax.random.fold_in(key, 11), (D, VOCAB), jnp.float32) * (1.0 / D) ** 0.5
    return values.astype(jnp.bfloat16).astype(jnp.float32)


def draw_proj_weight(key, part):
    return shared_weight(key).astype(jnp.bfloat16)


def draw_hidden(key, part):
    scale_key = jax.random.fold_in(key, 31)
    noise_key = jax.random.fold_in(key, 32)
    subset_pos = (jnp.arange(TOKEN_ROW_COUNT) // ROWS).astype(jnp.float32)
    scales = 3.0 ** (subset_pos / max(SUBSETS - 1, 1)) * jax.random.uniform(scale_key, (TOKEN_ROW_COUNT,), jnp.float32, 0.7, 1.4)
    noise = jax.random.normal(noise_key, (TOKEN_ROW_COUNT, D), jnp.float32)
    values = noise * scales[:, None]
    return values.astype(jnp.bfloat16)


def draw_counts(key, part):
    row_offsets = jax.random.randint(jax.random.fold_in(key, 41), (SUBSETS, RESAMPLES, ROWS), 0, SUBSETS)
    shuffled = jax.random.permutation(jax.random.fold_in(key, 42), row_offsets, axis=2, independent=True)
    return (SUBSETS + row_offsets - shuffled).astype(jnp.int32)


def touch_ends(result, own_key, low, largest):
    dims = result.shape
    place = [jax.random.randint(jax.random.fold_in(own_key, axis), (), 0, dims[axis]) for axis in range(len(dims))]
    result = result.at[tuple(place)].set(low)
    longest = dims.index(max(dims))
    place[longest] = (place[longest] + 1) % dims[longest]
    return result.at[tuple(place)].set(largest)


def setup_inputs(seed: int = 0) -> dict:
    seeds = jax.random.split(jax.random.key(seed), 6)
    return {
        "hidden": draw_hidden(jax.random.fold_in(seeds[5], 71), 0),
        "proj_weight": draw_proj_weight(jax.random.fold_in(seeds[5], 71), 0),
        "targets": touch_ends(jax.random.randint(seeds[2], (TOKEN_ROW_COUNT,), 0, VOCAB), jax.random.fold_in(seeds[2], 1), 0, VOCAB - 1).astype(jnp.int32),
        "counts": draw_counts(jax.random.fold_in(seeds[5], 71), 0),
        "ranks": touch_ends(jax.random.randint(seeds[4], (QUANT,), 0, SUBSETS * RESAMPLES), jax.random.fold_in(seeds[4], 1), 0, (SUBSETS * RESAMPLES) - 1).astype(jnp.int32),
    }


def reference(hidden, proj_weight, targets, counts, ranks):
    def subset_loss(inputs):
        block_rows, block_targets = inputs
        logit_scores = jnp.dot(block_rows, proj_weight, preferred_element_type=jnp.float32)
        row_max = jnp.max(logit_scores, axis=1)
        row_total = jnp.sum(jnp.exp(logit_scores - row_max[:, None]), axis=1)
        picked = jnp.take_along_axis(logit_scores, block_targets[:, None].astype(jnp.int32), axis=1)[:, 0]
        return row_max + jnp.log(row_total) - picked

    stacked_values = lax.map(subset_loss, (hidden.reshape(SUBSETS, ROWS, D), targets.reshape(SUBSETS, ROWS)))
    row_cross_entropy = stacked_values.reshape(TOKEN_ROW_COUNT)
    resample_mean_losses = jnp.einsum("kjd,kd->kj", counts.astype(jnp.float32), stacked_values, precision=lax.Precision.HIGHEST) / (1.0 * TOKEN_ROW_COUNT)
    pooled = jnp.sort(resample_mean_losses.reshape(SUBSETS * RESAMPLES))
    positions = lax.iota(jnp.int32, SUBSETS * RESAMPLES)
    chosen = positions[:, None] == ranks[None, :]
    quantiles = jnp.sum(jnp.where(chosen, pooled[:, None], 0.0), axis=0)
    return row_cross_entropy, resample_mean_losses, quantiles
```

```python
import functools
import math

import jax
import jax.numpy as jnp
from jax import lax
from jax.experimental import pallas as pl
from jax.experimental.pallas import tpu as pltpu
from jax.sharding import PartitionSpec as P


VMEM_LIMIT = 60_000_000
CHUNK_SHARES = (8, 8, 6, 3)


def pooled_groups(subsets, rows, columns):
    fits = [n for n in range(1, subsets + 1) if subsets % n == 0 and columns % (16 * n) == 0]
    return min(fits, key=lambda n: n * rows + columns // n)


def chunk_sizes(columns):
    units, total = columns // 16, sum(CHUNK_SHARES)
    ends = [units * sum(CHUNK_SHARES[: n + 1]) // total for n in range(len(CHUNK_SHARES))]
    sizes = [16 * (b - a) for a, b in zip([0] + ends[:-1], ends)]
    return [n for n in sizes if n]


def split_kernel(pool, width, sizes, place_ref, weight_ref, *refs):
    n_out = 1 + (pool - 1) * len(sizes)
    outs, (turned, sems) = refs[:n_out], refs[n_out:]
    turned[...] = weight_ref[...].T
    starts = [(0, 0, width)]
    for k in range(1, pool):
        offset = 0
        for size in sizes:
            starts.append((k, offset, size))
            offset += size
    order = sorted(range(n_out), key=lambda n: (starts[n][1], starts[n][0]))
    copies = []
    for n in order:
        k, offset, size = starts[n]
        target = lax.rem(place_ref[0] + k, pool)
        begin = pl.multiple_of(target * width + offset, 16)
        copies.append(pltpu.make_async_copy(turned.at[pl.ds(begin, size), :], outs[n], sems.at[n]))
    for copy in copies:
        copy.start()
    for copy in copies:
        copy.wait()


def score_kernel(pool, size, offset, n_w, n_h, w_slices, first, last, place_ref, *refs):
    targets, refs = refs[:pool], refs[pool:]
    if first:
        before = None
    else:
        before, refs = refs[0], refs[1:]
    w_refs, h_refs, refs = refs[:n_w], refs[n_w : n_w + n_h], refs[n_w + n_h :]
    if last:
        outs, refs = refs[:pool], refs[pool:]
    else:
        outs, refs = refs[:1], refs[1:]
    w_buf, h_buf, wanted, state, w_sems, h_sems = refs
    rows = h_buf.shape[1]
    w_copies, h_copies = [], []
    for n, ref in enumerate(w_refs):
        lanes = pl.ds(pl.multiple_of(place_ref[1 + n], 128), ref.shape[1])
        source = ref.at[pl.ds(offset, size), :] if w_slices[n] else ref
        w_copies.append(pltpu.make_async_copy(source, w_buf.at[:, lanes], w_sems.at[n]))
    for n, ref in enumerate(h_refs):
        slot = place_ref[1 + n_w + 2 * n]
        lanes = pl.ds(pl.multiple_of(place_ref[2 + n_w + 2 * n], 128), ref.shape[1])
        h_copies.append(pltpu.make_async_copy(ref, h_buf.at[slot, :, lanes], h_sems.at[n]))
    for copy in w_copies + h_copies:
        copy.start()
    base = place_ref[1 + n_w + 2 * n_h]
    for k in range(pool):
        wanted[lax.rem(place_ref[0] - k + pool, pool)] = targets[k][...] - (base + offset)
    for copy in w_copies:
        copy.wait()
    per = n_h // pool
    for j in range(pool):
        for copy in h_copies[per * j : per * (j + 1)]:
            copy.wait()
        slot = place_ref[1 + n_w + 2 * per * j]
        logits = lax.dot_general(
            w_buf[...], h_buf[slot], (((1,), (1,)), ((), ())), preferred_element_type=jnp.float32
        )
        top = jnp.max(logits, axis=0, keepdims=True)
        hit = lax.broadcasted_iota(jnp.int32, logits.shape, 0) == wanted[slot]
        picked = jnp.sum(jnp.where(hit, logits, 0.0), axis=0, keepdims=True)
        if not first:
            old_top = before[slot, 0:1, :]
            new_top = jnp.maximum(old_top, top)
            total = before[slot, 1:2, :] * jnp.exp(old_top - new_top)
            picked = picked + before[slot, 2:3, :]
        else:
            new_top, total = top, 0.0
        total = total + jnp.sum(jnp.exp(logits - new_top), axis=0, keepdims=True)
        state[slot, 0:1, :] = new_top
        state[slot, 1:2, :] = total
        state[slot, 2:3, :] = picked
    if last:
        for k in range(pool):
            outs[k][...] = state[lax.rem(place_ref[0] + k, pool)]
    else:
        outs[0][...] = state[...]


def merge(parts):
    top = functools.reduce(jnp.maximum, [p[0:1, :] for p in parts])
    total = sum(p[1:2, :] * jnp.exp(p[0:1, :] - top) for p in parts)
    return top, total, sum(p[2:3, :] for p in parts)


def merge_kernel(*refs):
    out = refs[-1]
    top, total, picked = merge([r[...] for r in refs[:-1]])
    out[0:1, :] = top
    out[1:2, :] = total
    out[2:3, :] = picked


def loss_kernel(n_parts, n_counts, total_rows, *refs):
    parts, counts, outs = refs[:n_parts], refs[n_parts : n_parts + n_counts], refs[n_parts + n_counts :]
    ce_ref, own_ref, all_ref = outs
    top, total, picked = merge([r[...] for r in parts])
    loss = top + jnp.log(total) - picked
    ce_ref[...] = loss
    per = own_ref.shape[1]
    lanes = []
    for n, ref in enumerate(counts):
        means = lax.dot_general(
            loss, ref[...].astype(jnp.float32), (((1,), (1,)), ((), ())),
            precision=lax.Precision.HIGHEST, preferred_element_type=jnp.float32,
        ) / total_rows
        if n == 0:
            own_ref[...] = means
        lanes.append(means)
    row = jnp.concatenate(lanes, axis=1)
    for n in range(all_ref.shape[0]):
        all_ref[n] = row


def rank_kernel(n_ranks, ranks_ref, values_ref, out_ref):
    groups, _, width = values_ref.shape
    shape = (width, width)
    diagonal = lax.broadcasted_iota(jnp.int32, shape, 0) == lax.broadcasted_iota(jnp.int32, shape, 1)

    def one(n, best):
        mine = values_ref[n]
        column = jnp.sum(jnp.where(diagonal, mine, 0.0), axis=1, keepdims=True)

        def count(m, sums):
            other = values_ref[m]
            return sums[0] + jnp.where(other < column, 1.0, 0.0), sums[1] + jnp.where(other <= column, 1.0, 0.0)

        zero = jnp.zeros(shape, jnp.float32)
        below, upto = lax.fori_loop(0, groups, count, (zero, zero), unroll=min(groups, 8))
        below = jnp.sum(below, axis=1, keepdims=True)
        upto = jnp.sum(upto, axis=1, keepdims=True)
        rank = ranks_ref[...].astype(jnp.float32)
        hit = (below <= rank) & (rank < upto)
        return jnp.maximum(best, jnp.max(jnp.where(hit, column, -jnp.inf), axis=0, keepdims=True))

    out_ref[...] = lax.fori_loop(0, groups, one, jnp.full((1, n_ranks), -jnp.inf, jnp.float32))


ANY = pl.BlockSpec(memory_space=pl.ANY)
VMEM = pl.BlockSpec(memory_space=pltpu.VMEM)
SMEM = pl.BlockSpec(memory_space=pltpu.SMEM)
PARAMS = pltpu.CompilerParams(vmem_limit_bytes=VMEM_LIMIT)


def body(subsets, groups, hidden, proj_weight, targets, counts, ranks):
    rows, depth = hidden.shape
    share, columns = proj_weight.shape
    resamples = counts.shape[1]
    pool = pooled_groups(subsets, rows, columns)
    inner = subsets // pool
    width = columns // pool
    sizes = chunk_sizes(width)
    subset, group = lax.axis_index("subset"), lax.axis_index("vocab")
    place, member = subset // inner, subset % inner

    def along(x, step):
        pairs = [(a * inner + b, step(a) * inner + b) for a in range(pool) for b in range(inner) if step(a) is not None]
        return lax.ppermute(x, "subset", pairs)

    def across(x, flip):
        return lax.ppermute(x, "vocab", [(a, a ^ flip) for a in range(groups)])

    def swap(x):
        return lax.ppermute(x, "subset", [(a, a ^ 1) for a in range(subsets)])

    def shift(x, k):
        return along(x, lambda a: (a + k) % pool)

    if pool == 4 and groups == 4:
        near = along(hidden, lambda a: a ^ 1)
        middle = along(hidden, {0: None, 1: 2, 2: 1, 3: None}.get)
        outward = {0: None, 1: 0, 2: 3, 3: None}.get
        middle_near = along(near, {0: None, 1: 2, 2: 1, 3: None}.get)
        is_middle = (place == 1) | (place == 2)
        third = jnp.where(is_middle, middle, along(middle, outward))
        fourth = jnp.where(is_middle, middle_near, along(middle_near, outward))
        low = place < 2
        slots = [place, place ^ 1, jnp.where(low, 2, 1), jnp.where(low, 3, 0)]
        h_refs, h_places = [], []
        for piece, slot in zip((hidden, near, third, fourth), slots):
            over = across(piece, 2)
            for flip, part in ((0, piece), (2, over), (1, across(piece, 1)), (3, across(over, 1))):
                h_refs.append(part)
                h_places += [slot, (group ^ flip) * depth]
    else:
        index = [[a * inner + b for a in range(pool)] for b in range(inner)]
        whole = lax.all_gather(hidden, "subset", axis_index_groups=index)
        whole = lax.all_gather(whole, "vocab", axis=2, tiled=True)
        h_refs = [whole[n] for n in range(pool)]
        h_places = [x for n in range(pool) for x in (jnp.int32(n), jnp.int32(0))]

    n_out = 1 + (pool - 1) * len(sizes)
    pieces = pl.pallas_call(
        functools.partial(split_kernel, pool, width, sizes),
        out_shape=[jax.ShapeDtypeStruct((width, share), proj_weight.dtype)]
        + [jax.ShapeDtypeStruct((n, share), proj_weight.dtype) for _ in range(1, pool) for n in sizes],
        in_specs=[SMEM, VMEM],
        out_specs=[ANY] * n_out,
        scratch_shapes=[pltpu.VMEM((columns, share), proj_weight.dtype), pltpu.SemaphoreType.DMA((n_out,))],
        compiler_params=PARAMS,
        name="split",
    )(place[None], proj_weight)
    own = pieces[0]

    def gather_inner(x):
        if inner == 1:
            return [(x, 0)]
        if inner == 2:
            return [(x, member * share), (swap(x), (1 - member) * share)]
        index = [[a * inner + b for b in range(inner)] for a in range(pool)]
        return [(lax.all_gather(x, "subset", axis=1, tiled=True, axis_index_groups=index), 0)]

    target_parts = [targets[None]] + [shift(targets[None], k) for k in range(1, pool)]
    own_parts = gather_inner(own)
    base = group * columns + place * width
    state, offset = None, 0
    for n, size in enumerate(sizes):
        first, last = n == 0, n == len(sizes) - 1
        block = inner * share
        w = [(x, place * block + at, True) for x, at in own_parts]
        for k in range(1, pool):
            source = lax.rem(place - k + pool, pool)
            came = shift(pieces[1 + (k - 1) * len(sizes) + n], k)
            w += [(x, source * block + at, False) for x, at in gather_inner(came)]
        scalars = jnp.stack([jnp.asarray(s, jnp.int32) for s in [place] + [at for _, at, _ in w] + h_places + [base]])
        n_w, n_h = len(w), len(h_refs)
        full = subsets * share
        row = jax.ShapeDtypeStruct((8, rows), jnp.float32)
        result = pl.pallas_call(
            functools.partial(score_kernel, pool, size, offset, n_w, n_h, [s for _, _, s in w], first, last),
            out_shape=[row] * pool if last else [jax.ShapeDtypeStruct((pool, 8, rows), jnp.float32)],
            in_specs=[SMEM] + [VMEM] * pool + ([] if first else [VMEM]) + [ANY] * (n_w + n_h),
            out_specs=[VMEM] * (pool if last else 1),
            scratch_shapes=[
                pltpu.VMEM((size, full), proj_weight.dtype),
                pltpu.VMEM((pool, rows, full), hidden.dtype),
                pltpu.VMEM((pool, 1, rows), jnp.int32),
                pltpu.VMEM((pool, 8, rows), jnp.float32),
                pltpu.SemaphoreType.DMA((n_w,)),
                pltpu.SemaphoreType.DMA((n_h,)),
            ],
            compiler_params=PARAMS,
            cost_estimate=pl.CostEstimate(
                flops=2 * pool * rows * full * size, bytes_accessed=2 * full * (pool * rows + size), transcendentals=pool * rows * size
            ),
            name=f"score{n}",
        )(scalars, *target_parts, *([] if first else [state]), *[x for x, _, _ in w], *h_refs)
        if last:
            mine = result
        else:
            state = result[0]
        offset += size

    row = jax.ShapeDtypeStruct((8, rows), jnp.float32)
    parts = [mine[0]] + [shift(mine[k], k) for k in range(1, pool)]
    merged = pl.pallas_call(merge_kernel, out_shape=row, name="merge")(*parts)
    narrow = counts[0].astype(jnp.bfloat16)
    if groups & (groups - 1) == 0:
        parts = [merged] + [across(merged, k) for k in range(1, groups)]
        all_counts = [counts[0]] + [across(narrow, k) for k in range(1, groups)]
    else:
        every = lax.all_gather(merged, "vocab")
        parts = [every[n] for n in range(groups)]
        every = lax.all_gather(narrow, "vocab")
        all_counts = [counts[0]] + [every[lax.rem(group + k, groups)] for k in range(1, groups)]
    loss, means, spread = pl.pallas_call(
        functools.partial(loss_kernel, len(parts), groups, float(subsets * rows)),
        out_shape=[
            jax.ShapeDtypeStruct((1, rows), jnp.float32),
            jax.ShapeDtypeStruct((1, resamples), jnp.float32),
            jax.ShapeDtypeStruct((subsets, 1, groups * resamples), jnp.float32),
        ],
        name="losses",
    )(*parts, *all_counts)
    pooled = lax.all_to_all(spread, "subset", 0, 0)
    quantiles = pl.pallas_call(
        functools.partial(rank_kernel, ranks.shape[0]),
        out_shape=jax.ShapeDtypeStruct((1, ranks.shape[0]), jnp.float32),
        name="ranks",
    )(ranks[None], pooled)
    return loss[0], means, quantiles[0]


def solution(mesh):
    return jax.shard_map(
        functools.partial(body, mesh.shape["subset"], mesh.shape["vocab"]),
        mesh=mesh,
        in_specs=(
            P("subset", "vocab"),
            P("subset", "vocab"),
            P("subset"),
            P("subset", "vocab", None),
            P(),
        ),
        out_specs=(P("subset"), P("subset", "vocab"), P()),
        check_vma=False,
    )
```

```python
import functools

import jax
import jax.numpy as jnp
from jax import lax
from jax.experimental import pallas as pl
from jax.experimental.pallas import tpu as pltpu
from jax.sharding import PartitionSpec as P


CHUNK_SHARES = (26, 30, 28, 16)
POOL = 4
BASE = 256
DIGIT_ROWS = 16
LANES = 128
ANY = pl.BlockSpec(memory_space=pl.ANY)
HBM = pl.BlockSpec(memory_space=pltpu.HBM)
VMEM = pl.BlockSpec(memory_space=pltpu.VMEM)
SMEM = pl.BlockSpec(memory_space=pltpu.SMEM)
PARAMS = pltpu.CompilerParams(vmem_limit_bytes=24_000_000)
WIDE = pltpu.CompilerParams(vmem_limit_bytes=62_000_000)


def chunk_sizes(columns):
    units, total = columns // 16, sum(CHUNK_SHARES)
    ends = [units * sum(CHUNK_SHARES[: n + 1]) // total for n in range(len(CHUNK_SHARES))]
    return [16 * (b - a) for a, b in zip([0] + ends[:-1], ends)]


def split_kernel(width, sizes, extra_rows, place_ref, weight_ref, extra_ref, *refs):
    n_out = 1 + (POOL - 1) * len(sizes)
    outs, (turned, sems) = refs[:n_out], refs[n_out:]
    turned[...] = weight_ref[...].T
    pieces = [(0, 0, 0, width)]
    for n, size in enumerate(sizes):
        for k in range(1, POOL):
            pieces.append((1 + (k - 1) * len(sizes) + n, k, sum(sizes[:n]), size))
    copies = []

    def copy(source, target):
        copies.append(pltpu.make_async_copy(source, target, sems.at[len(copies)]))

    for n, k, offset, size in pieces:
        begin = pl.multiple_of(lax.rem(place_ref[0] + k, POOL) * width + offset, 16)
        copy(turned.at[pl.ds(begin, size), :], outs[n].at[pl.ds(0, size), :])
        if k and not offset:
            copy(extra_ref, outs[n].at[pl.ds(size, extra_rows), :])
    for c in copies:
        c.start()
    for c in copies:
        c.wait()


def gather_kernel(groups, rows, depth, count_rows, place_ref, *refs):
    n_parts = (POOL + 1) * groups
    parts, (hidden, counts, digits, sems) = refs[:n_parts], refs[n_parts:]
    copies = []

    def copy(ref, begin, size, target):
        copies.append(pltpu.make_async_copy(ref.at[pl.ds(begin, size), :], target, sems.at[len(copies)]))

    for n, ref in enumerate(parts[: POOL * groups]):
        slot, flip = n // groups, n % groups
        lanes = pl.ds(pl.multiple_of(place_ref[POOL + flip], LANES), depth)
        copy(ref, 0, rows, hidden.at[place_ref[slot], :, lanes])
    for flip in range(groups):
        for k in range(POOL):
            member = lax.rem(place_ref[0] - k + POOL, POOL)
            begin = k * (count_rows + DIGIT_ROWS)
            carrier = parts[POOL * groups + flip]
            copy(carrier, begin, count_rows, counts.at[member, pl.ds(flip * count_rows, count_rows), :])
            if flip == 0:
                copy(carrier, begin + count_rows, DIGIT_ROWS, digits.at[member])
    for c in copies:
        c.start()
    for c in copies:
        c.wait()


def score_kernel(size, offset, n_w, sliced, first, place_ref, digits, *refs):
    before, refs = (None, refs) if first else (refs[0], refs[1:])
    w_refs, (hidden, out, w_buf, w_sems) = refs[:n_w], refs[n_w:]
    copies = []
    for n, ref in enumerate(w_refs):
        lanes = pl.ds(pl.multiple_of(place_ref[1 + n], LANES), ref.shape[1])
        source = ref.at[pl.ds(offset if sliced[n] else 0, size), :]
        copies.append(pltpu.make_async_copy(source, w_buf.at[:, lanes], w_sems.at[n]))
    for copy in copies:
        copy.start()
    for copy in copies:
        copy.wait()
    for z in range(POOL):
        number = digits[z, 0:3, :].astype(jnp.float32)
        wanted = (number[0:1] * BASE + number[1:2]) * BASE + number[2:3]
        wanted = wanted.astype(jnp.int32) - (place_ref[0] + offset)
        logits = lax.dot_general(
            w_buf[...], hidden[z], (((1,), (1,)), ((), ())), preferred_element_type=jnp.float32
        )
        top = jnp.max(logits, axis=0, keepdims=True)
        hit = lax.broadcasted_iota(jnp.int32, logits.shape, 0) == wanted
        picked = jnp.sum(jnp.where(hit, logits, 0.0), axis=0, keepdims=True)
        if first:
            total = jnp.sum(jnp.exp(logits - top), axis=0, keepdims=True)
        else:
            old = before[z : z + 1, :]
            top = jnp.maximum(old, top)
            total = before[POOL + z : POOL + z + 1, :] * jnp.exp(old - top)
            total = total + jnp.sum(jnp.exp(logits - top), axis=0, keepdims=True)
            picked = picked + before[2 * POOL + z : 2 * POOL + z + 1, :]
        out[z : z + 1, :] = top
        out[POOL + z : POOL + z + 1, :] = total
        out[2 * POOL + z : 2 * POOL + z + 1, :] = picked


def merge(parts):
    tops = [p[0:POOL] for p in parts]
    top = functools.reduce(jnp.maximum, tops)
    total = sum(p[POOL : 2 * POOL] * jnp.exp(t - top) for p, t in zip(parts, tops))
    return top, total, sum(p[2 * POOL : 3 * POOL] for p in parts)


def merge_kernel(*refs):
    top, total, picked = merge([r[...] for r in refs[:-1]])
    refs[-1][...] = jnp.concatenate([top, total, picked], axis=0)


def loss_kernel(n_parts, total_rows, place_ref, *refs):
    parts, (counts, loss_ref, own_ref, means_ref, losses) = refs[:n_parts], refs[n_parts:]
    top, total, picked = merge([r[...] for r in parts])
    losses[...] = top + jnp.log(total) - picked
    loss_ref[...] = losses[pl.ds(place_ref[0], 1), :]
    for z in range(POOL):
        rest, thirds = losses[z : z + 1, :], []
        for _ in range(3):
            thirds.append(rest.astype(jnp.bfloat16))
            rest = rest - thirds[-1].astype(jnp.float32)
        sums = lax.dot_general(
            jnp.concatenate(thirds, axis=0), counts[z], (((1,), (1,)), ((), ())), preferred_element_type=jnp.float32
        )
        means_ref[z : z + 1, :] = jnp.sum(sums, axis=0, keepdims=True) / total_rows
    own_ref[...] = means_ref[pl.ds(place_ref[0], 1), 0 : own_ref.shape[1]]


def rank_kernel(resamples, count_rows, ranks_ref, *refs):
    parts, (out_ref, values) = refs[:-2], refs[-2:]
    width = parts[0].shape[1]
    lane = lax.broadcasted_iota(jnp.int32, (POOL, width), 1)
    valid = lax.rem(lane, count_rows) < resamples
    for n, part in enumerate(parts):
        kept = jnp.where(valid, part[...], jnp.inf)
        for z in range(POOL):
            values[n * POOL + z] = kept[z : z + 1]
    groups = values.shape[0]
    shape = (width, width)
    diagonal = lax.broadcasted_iota(jnp.int32, shape, 0) == lax.broadcasted_iota(jnp.int32, shape, 1)
    rank = ranks_ref[...].astype(jnp.float32)

    def one(n, best):
        column = jnp.sum(jnp.where(diagonal, values[n], 0.0), axis=1, keepdims=True)
        below = lax.fori_loop(
            0,
            groups,
            lambda m, c: c + jnp.where(values[m] < column, 1.0, 0.0),
            jnp.zeros(shape, jnp.float32),
            unroll=min(groups, 8),
        )
        below = jnp.sum(below, axis=1, keepdims=True)
        return jnp.maximum(best, jnp.max(jnp.where(below <= rank, column, -jnp.inf), axis=0, keepdims=True))

    start = jnp.full(rank.shape, -jnp.inf, jnp.float32)
    out_ref[...] = lax.fori_loop(0, groups, one, start, unroll=min(groups, 2))


def pooled(subsets, groups, hidden, proj_weight, targets, counts, ranks):
    rows, depth = hidden.shape
    share, columns = proj_weight.shape
    resamples = counts.shape[1]
    inner = subsets // POOL
    width = columns // POOL
    full = subsets * share
    sizes = chunk_sizes(width)
    subset, group = lax.axis_index("subset"), lax.axis_index("vocab")
    place, member = subset // inner, subset % inner

    def along(x, step):
        pairs = [(a * inner + b, step(a) * inner + b) for a in range(POOL) for b in range(inner) if step(a) is not None]
        return lax.ppermute(x, "subset", pairs)

    def across(x, flip):
        return lax.ppermute(x, "vocab", [(a, a ^ flip) for a in range(groups)])

    def shift(x, k):
        return along(x, lambda a: (a + k) % POOL)

    count_rows = -(-resamples // 16) * 16
    narrow = jnp.pad(counts[0].astype(jnp.bfloat16), ((0, count_rows - resamples), (0, 0)))
    digits = jnp.stack([targets // (BASE * BASE), targets // BASE % BASE, targets % BASE])
    digits = jnp.pad(digits.astype(jnp.bfloat16), ((0, DIGIT_ROWS - 3), (0, 0)))
    extra = jnp.concatenate([narrow, digits], axis=0)
    spread = extra.reshape(-1, share)
    extra_rows = spread.shape[0]
    middle = {0: None, 1: 2, 2: 1, 3: None}.get
    outward = {0: None, 1: 0, 2: 3, 3: None}.get
    near = along(hidden, lambda a: a ^ 1)
    mid = along(hidden, middle)
    mid_near = along(near, middle)
    is_middle = (place == 1) | (place == 2)
    outer, outer_near = along(mid, outward), along(mid_near, outward)
    third = jnp.where(is_middle, mid, outer)
    fourth = jnp.where(is_middle, mid_near, outer_near)
    low = place < 2
    slots = [place, place ^ 1, jnp.where(low, 2, 1), jnp.where(low, 3, 0)]
    parts = []
    for piece in (hidden, near, third, fourth):
        over = across(piece, 2)
        parts += [piece, across(piece, 1), over, across(over, 1)]
    n_out = 1 + (POOL - 1) * len(sizes)
    pieces = pl.pallas_call(
        functools.partial(split_kernel, width, sizes, extra_rows),
        out_shape=[jax.ShapeDtypeStruct((width, share), proj_weight.dtype)]
        + [
            jax.ShapeDtypeStruct((size + (0 if n else extra_rows), share), proj_weight.dtype)
            for _ in range(1, POOL)
            for n, size in enumerate(sizes)
        ],
        in_specs=[SMEM, VMEM, VMEM],
        out_specs=[HBM] * n_out,
        scratch_shapes=[pltpu.VMEM((columns, share), proj_weight.dtype), pltpu.SemaphoreType.DMA((n_out + POOL - 1,))],
        compiler_params=WIDE,
        cost_estimate=pl.CostEstimate(flops=10**9, bytes_accessed=4 * columns * share, transcendentals=0),
        name="split",
    )(place[None], proj_weight, spread)

    came = {}
    for n in range(len(sizes)):
        for k in range(1, POOL):
            came[n, k] = shift(pieces[1 + (k - 1) * len(sizes) + n], k)
    *late, _ = lax.optimization_barrier((*(came[0, k] for k in range(1, POOL)), parts[2 * groups + 2]))
    extras = [extra] + [x[sizes[0] :].reshape(extra.shape) for x in late]
    extra = lax.optimization_barrier(jnp.concatenate(extras, axis=0))
    parts += [extra] + [across(extra, flip) for flip in range(1, groups)]
    scalars = [*slots, *((group ^ flip) * depth for flip in range(groups))]
    hidden_all, counts_all, digits_all = pl.pallas_call(
        functools.partial(gather_kernel, groups, rows, depth, count_rows),
        out_shape=[
            jax.ShapeDtypeStruct((POOL, rows, groups * depth), hidden.dtype),
            jax.ShapeDtypeStruct((POOL, groups * count_rows, rows), jnp.bfloat16),
            jax.ShapeDtypeStruct((POOL, DIGIT_ROWS, rows), jnp.bfloat16),
        ],
        in_specs=[SMEM] + [ANY] * len(parts),
        out_specs=[VMEM] * 3,
        scratch_shapes=[pltpu.SemaphoreType.DMA((POOL * (2 * groups + 1),))],
        compiler_params=PARAMS,
        cost_estimate=pl.CostEstimate(flops=10**9, bytes_accessed=2 * POOL * rows * full, transcendentals=0),
        name="gather",
    )(jnp.stack([jnp.asarray(s, jnp.int32) for s in scalars]), *parts)

    def gather_inner(x):
        if inner == 1:
            return [(x, 0)]
        if inner == 2:
            other = lax.ppermute(x, "subset", [(a, a ^ 1) for a in range(subsets)])
            return [(x, member * share), (other, (1 - member) * share)]
        index = [[a * inner + b for b in range(inner)] for a in range(POOL)]
        return [(lax.all_gather(x, "subset", axis=1, tiled=True, axis_index_groups=index), 0)]

    own_parts = gather_inner(pieces[0])
    base = group * columns + place * width
    state, offset = None, 0
    for n, size in enumerate(sizes):
        block = inner * share
        w = [(x, place * block + at, True) for x, at in own_parts]
        for k in range(1, POOL):
            source = lax.rem(place - k + POOL, POOL)
            w += [(x, source * block + at, False) for x, at in gather_inner(came[n, k])]
        scalars = jnp.stack([jnp.asarray(s, jnp.int32) for s in [base] + [at for _, at, _ in w]])
        state = pl.pallas_call(
            functools.partial(score_kernel, size, offset, len(w), [s for _, _, s in w], n == 0),
            out_shape=jax.ShapeDtypeStruct((3 * POOL, rows), jnp.float32),
            in_specs=[SMEM, VMEM] + ([VMEM] if n else []) + [ANY] * len(w) + [VMEM],
            out_specs=VMEM,
            scratch_shapes=[pltpu.VMEM((size, full), proj_weight.dtype), pltpu.SemaphoreType.DMA((len(w),))],
            compiler_params=PARAMS,
            cost_estimate=pl.CostEstimate(
                flops=2 * POOL * rows * full * size, bytes_accessed=2 * full * size, transcendentals=POOL * rows * size
            ),
        )(scalars, digits_all, *([state] if n else []), *[x for x, _, _ in w], hidden_all)
        offset += size

    parts = [state] + [across(state, k) for k in range(1, groups)]
    merged = pl.pallas_call(
        merge_kernel, out_shape=jax.ShapeDtypeStruct((3 * POOL, rows), jnp.float32), name="merge"
    )(*parts)
    parts = [merged] + [shift(merged, k) for k in range(1, POOL)]
    loss, own, means = pl.pallas_call(
        functools.partial(loss_kernel, POOL, float(subsets * rows)),
        out_shape=[
            jax.ShapeDtypeStruct((1, rows), jnp.float32),
            jax.ShapeDtypeStruct((1, resamples), jnp.float32),
            jax.ShapeDtypeStruct((POOL, groups * count_rows), jnp.float32),
        ],
        in_specs=[SMEM] + [VMEM] * (POOL + 1),
        scratch_shapes=[pltpu.VMEM((POOL, rows), jnp.float32)],
        name="losses",
    )(place[None], *parts, counts_all)
    if inner == 1:
        values = [means]
    elif inner == 2:
        values = [means, lax.ppermute(means, "subset", [(a, a ^ 1) for a in range(subsets)])]
    else:
        index = [[a * inner + b for b in range(inner)] for a in range(POOL)]
        every = lax.all_gather(means, "subset", axis_index_groups=index)
        values = [every[n] for n in range(inner)]
    quantiles = pl.pallas_call(
        functools.partial(rank_kernel, resamples, count_rows),
        out_shape=jax.ShapeDtypeStruct((1, ranks.shape[0]), jnp.float32),
        scratch_shapes=[pltpu.VMEM((POOL * inner, 1, groups * count_rows), jnp.float32)],
        name="ranks",
    )(ranks[None], *values)
    return loss[0], own, quantiles[0]


def plain(hidden, proj_weight, targets, counts, ranks):
    features = lax.all_gather(hidden, "vocab", axis=1, tiled=True)
    columns = proj_weight.shape[1]
    whole_weight = lax.all_gather(proj_weight, "subset", axis=0, tiled=True)
    logits = jnp.dot(features, whole_weight, preferred_element_type=jnp.float32)
    local_top = jnp.max(logits, axis=1)
    local_sum = jnp.sum(jnp.exp(logits - local_top[:, None]), axis=1)
    offset = targets - lax.axis_index("vocab") * columns
    hit = lax.iota(jnp.int32, columns)[None, :] == offset[:, None]
    picked = jnp.sum(jnp.where(hit, logits, 0.0), axis=1)
    top = lax.pmax(local_top, "vocab")
    total, target_logit = lax.psum((local_sum * jnp.exp(local_top - top), picked), "vocab")
    loss = top + jnp.log(total) - target_logit
    total_rows = 1.0 * lax.axis_size("subset") * loss.shape[0]
    means = (
        jnp.einsum("cno,o->cn", counts.astype(jnp.float32), loss, precision=lax.Precision.HIGHEST) / total_rows
    )
    grouped = lax.all_gather(means, "vocab", axis=1, tiled=True)
    values = jnp.sort(lax.all_gather(grouped, "subset", axis=0, tiled=True).reshape(-1))
    chosen = lax.iota(jnp.int32, values.shape[0])[:, None] == ranks[None, :]
    return loss, means, jnp.sum(jnp.where(chosen, values[:, None], 0.0), axis=0)


def solution(mesh):
    subsets, groups = mesh.shape["subset"], mesh.shape["vocab"]

    def body(hidden, proj_weight, targets, counts, ranks):
        rows, depth = hidden.shape
        columns = proj_weight.shape[1]
        fits = (
            subsets % POOL == 0
            and groups == 4
            and rows == depth
            and rows % proj_weight.shape[0] == 0
            and rows % LANES == 0
            and columns % (16 * POOL) == 0
            and counts.shape[1] <= LANES // groups
        )
        if not fits:
            return plain(hidden, proj_weight, targets, counts, ranks)
        return pooled(subsets, groups, hidden, proj_weight, targets, counts, ranks)

    return jax.shard_map(
        body,
        mesh=mesh,
        in_specs=(
            P("subset", "vocab"),
            P("subset", "vocab"),
            P("subset"),
            P("subset", "vocab", None),
            P(),
        ),
        out_specs=(P("subset"), P("subset", "vocab"), P()),
        check_vma=False,
    )
```

```python
import functools

import jax
import jax.numpy as jnp
from jax import lax
from jax.experimental import pallas as pl
from jax.experimental.pallas import tpu as pltpu
from jax.sharding import PartitionSpec as P


CHUNK_SHARES = (26, 30, 28, 16)
POOL = 4
BASE = 256
DIGIT_ROWS = 16
LANES = 128
HBM = pl.BlockSpec(memory_space=pltpu.HBM)
VMEM = pl.BlockSpec(memory_space=pltpu.VMEM)
SMEM = pl.BlockSpec(memory_space=pltpu.SMEM)
PARAMS = pltpu.CompilerParams(vmem_limit_bytes=24_000_000)
WIDE = pltpu.CompilerParams(vmem_limit_bytes=62_000_000)


def chunk_sizes(columns):
    units, total = columns // 16, sum(CHUNK_SHARES)
    ends = [units * sum(CHUNK_SHARES[: n + 1]) // total for n in range(len(CHUNK_SHARES))]
    return [16 * (b - a) for a, b in zip([0] + ends[:-1], ends)]


def split_kernel(width, sizes, extra_rows, place_ref, weight_ref, extra_ref, *refs):
    n_out = 1 + (POOL - 1) * len(sizes)
    outs, (turned, sems) = refs[:n_out], refs[n_out:]
    turned[...] = weight_ref[...].T
    pieces = [(0, 0, 0, width)]
    for n, size in enumerate(sizes):
        for k in range(1, POOL):
            pieces.append((1 + (k - 1) * len(sizes) + n, k, sum(sizes[:n]), size))
    copies = []

    def copy(source, target):
        copies.append(pltpu.make_async_copy(source, target, sems.at[len(copies)]))

    for n, k, offset, size in pieces:
        begin = pl.multiple_of(lax.rem(place_ref[0] + k, POOL) * width + offset, 16)
        copy(turned.at[pl.ds(begin, size), :], outs[n].at[pl.ds(0, size), :])
        if k and not offset:
            copy(extra_ref, outs[n].at[pl.ds(size, extra_rows), :])
    for c in copies:
        c.start()
    for c in copies:
        c.wait()


def gather_kernel(groups, rows, depth, count_rows, place_ref, *refs):
    n_parts = (POOL + 1) * groups
    parts, (hidden, counts, digits, sems) = refs[:n_parts], refs[n_parts:]
    copies = []

    def copy(ref, begin, size, target):
        copies.append(pltpu.make_async_copy(ref.at[pl.ds(begin, size), :], target, sems.at[len(copies)]))

    for n, ref in enumerate(parts[: POOL * groups]):
        slot, flip = n // groups, n % groups
        lanes = pl.ds(pl.multiple_of(place_ref[POOL + flip], LANES), depth)
        copy(ref, 0, rows, hidden.at[place_ref[slot], :, lanes])
    for flip in range(groups):
        for k in range(POOL):
            member = lax.rem(place_ref[0] - k + POOL, POOL)
            begin = k * (count_rows + DIGIT_ROWS)
            carrier = parts[POOL * groups + flip]
            copy(carrier, begin, count_rows, counts.at[member, pl.ds(flip * count_rows, count_rows), :])
            if flip == 0:
                copy(carrier, begin + count_rows, DIGIT_ROWS, digits.at[member])
    for c in copies:
        c.start()
    for c in copies:
        c.wait()


def score_kernel(size, offset, n_w, sliced, first, place_ref, digits, *refs):
    before, refs = (None, refs) if first else (refs[0], refs[1:])
    w_refs, (hidden, out, w_buf, w_sems) = refs[:n_w], refs[n_w:]
    copies = []
    for n, ref in enumerate(w_refs):
        lanes = pl.ds(pl.multiple_of(place_ref[1 + n], LANES), ref.shape[1])
        source = ref.at[pl.ds(offset if sliced[n] else 0, size), :]
        copies.append(pltpu.make_async_copy(source, w_buf.at[:, lanes], w_sems.at[n]))
    for copy in copies:
        copy.start()
    for copy in copies:
        copy.wait()
    for z in range(POOL):
        number = digits[z, 0:3, :].astype(jnp.float32)
        wanted = (number[0:1] * BASE + number[1:2]) * BASE + number[2:3]
        wanted = wanted.astype(jnp.int32) - (place_ref[0] + offset)
        logits = lax.dot_general(
            w_buf[...], hidden[z], (((1,), (1,)), ((), ())), preferred_element_type=jnp.float32
        )
        top = jnp.max(logits, axis=0, keepdims=True)
        hit = lax.broadcasted_iota(jnp.int32, logits.shape, 0) == wanted
        picked = jnp.sum(jnp.where(hit, logits, 0.0), axis=0, keepdims=True)
        if first:
            total = jnp.sum(jnp.exp(logits - top), axis=0, keepdims=True)
        else:
            old = before[z : z + 1, :]
            top = jnp.maximum(old, top)
            total = before[POOL + z : POOL + z + 1, :] * jnp.exp(old - top)
            total = total + jnp.sum(jnp.exp(logits - top), axis=0, keepdims=True)
            picked = picked + before[2 * POOL + z : 2 * POOL + z + 1, :]
        out[z : z + 1, :] = top
        out[POOL + z : POOL + z + 1, :] = total
        out[2 * POOL + z : 2 * POOL + z + 1, :] = picked


def merge(parts):
    tops = [p[0:POOL] for p in parts]
    top = functools.reduce(jnp.maximum, tops)
    total = sum(p[POOL : 2 * POOL] * jnp.exp(t - top) for p, t in zip(parts, tops))
    return top, total, sum(p[2 * POOL : 3 * POOL] for p in parts)


def merge_kernel(*refs):
    top, total, picked = merge([r[...] for r in refs[:-1]])
    refs[-1][...] = jnp.concatenate([top, total, picked], axis=0)


def loss_kernel(n_parts, total_rows, place_ref, *refs):
    parts, (counts, loss_ref, own_ref, means_ref, losses) = refs[:n_parts], refs[n_parts:]
    top, total, picked = merge([r[...] for r in parts])
    losses[...] = top + jnp.log(total) - picked
    loss_ref[...] = losses[pl.ds(place_ref[0], 1), :]
    for z in range(POOL):
        rest, thirds = losses[z : z + 1, :], []
        for _ in range(3):
            thirds.append(rest.astype(jnp.bfloat16))
            rest = rest - thirds[-1].astype(jnp.float32)
        sums = lax.dot_general(
            jnp.concatenate(thirds, axis=0), counts[z], (((1,), (1,)), ((), ())), preferred_element_type=jnp.float32
        )
        means_ref[z : z + 1, :] = jnp.sum(sums, axis=0, keepdims=True) / total_rows
    own_ref[...] = means_ref[pl.ds(place_ref[0], 1), 0 : own_ref.shape[1]]


def rank_kernel(resamples, count_rows, ranks_ref, *refs):
    parts, (out_ref, values) = refs[:-2], refs[-2:]
    width = parts[0].shape[1]
    lane = lax.broadcasted_iota(jnp.int32, (POOL, width), 1)
    valid = lax.rem(lane, count_rows) < resamples
    for n, part in enumerate(parts):
        kept = jnp.where(valid, part[...], jnp.inf)
        for z in range(POOL):
            values[n * POOL + z] = kept[z : z + 1]
    groups = values.shape[0]
    shape = (width, width)
    diagonal = lax.broadcasted_iota(jnp.int32, shape, 0) == lax.broadcasted_iota(jnp.int32, shape, 1)
    rank = ranks_ref[...].astype(jnp.float32)

    def one(n, best):
        column = jnp.sum(jnp.where(diagonal, values[n], 0.0), axis=1, keepdims=True)
        below = lax.fori_loop(
            0,
            groups,
            lambda m, c: c + jnp.where(values[m] < column, 1.0, 0.0),
            jnp.zeros(shape, jnp.float32),
            unroll=min(groups, 8),
        )
        below = jnp.sum(below, axis=1, keepdims=True)
        return jnp.maximum(best, jnp.max(jnp.where(below <= rank, column, -jnp.inf), axis=0, keepdims=True))

    start = jnp.full(rank.shape, -jnp.inf, jnp.float32)
    out_ref[...] = lax.fori_loop(0, groups, one, start, unroll=min(groups, 8))


def pooled(subsets, groups, hidden, proj_weight, targets, counts, ranks):
    rows, depth = hidden.shape
    share, columns = proj_weight.shape
    resamples = counts.shape[1]
    inner = subsets // POOL
    width = columns // POOL
    full = subsets * share
    sizes = chunk_sizes(width)
    subset, group = lax.axis_index("subset"), lax.axis_index("vocab")
    place, member = subset // inner, subset % inner

    def along(x, step):
        pairs = [(a * inner + b, step(a) * inner + b) for a in range(POOL) for b in range(inner) if step(a) is not None]
        return lax.ppermute(x, "subset", pairs)

    def across(x, flip):
        return lax.ppermute(x, "vocab", [(a, a ^ flip) for a in range(groups)])

    def shift(x, k):
        return along(x, lambda a: (a + k) % POOL)

    count_rows = -(-resamples // 16) * 16
    narrow = jnp.pad(counts[0].astype(jnp.bfloat16), ((0, count_rows - resamples), (0, 0)))
    digits = jnp.stack([targets // (BASE * BASE), targets // BASE % BASE, targets % BASE])
    digits = jnp.pad(digits.astype(jnp.bfloat16), ((0, DIGIT_ROWS - 3), (0, 0)))
    extra = jnp.concatenate([narrow, digits], axis=0)
    spread = extra.reshape(-1, share)
    extra_rows = spread.shape[0]
    middle = {0: None, 1: 2, 2: 1, 3: None}.get
    outward = {0: None, 1: 0, 2: 3, 3: None}.get
    near = along(hidden, lambda a: a ^ 1)
    mid = along(hidden, middle)
    mid_near = along(near, middle)
    is_middle = (place == 1) | (place == 2)
    outer, outer_near = along(mid, outward), along(mid_near, outward)
    third = jnp.where(is_middle, mid, outer)
    fourth = jnp.where(is_middle, mid_near, outer_near)
    low = place < 2
    slots = [place, place ^ 1, jnp.where(low, 2, 1), jnp.where(low, 3, 0)]
    parts = []
    for piece in (hidden, near, third, fourth):
        over = across(piece, 2)
        parts += [piece, across(piece, 1), over, across(over, 1)]
    n_out = 1 + (POOL - 1) * len(sizes)
    pieces = pl.pallas_call(
        functools.partial(split_kernel, width, sizes, extra_rows),
        out_shape=[jax.ShapeDtypeStruct((width, share), proj_weight.dtype)]
        + [
            jax.ShapeDtypeStruct((size + (0 if n else extra_rows), share), proj_weight.dtype)
            for _ in range(1, POOL)
            for n, size in enumerate(sizes)
        ],
        in_specs=[SMEM, VMEM, VMEM],
        out_specs=[HBM] * n_out,
        scratch_shapes=[pltpu.VMEM((columns, share), proj_weight.dtype), pltpu.SemaphoreType.DMA((n_out + POOL - 1,))],
        compiler_params=WIDE,
        cost_estimate=pl.CostEstimate(flops=10**9, bytes_accessed=4 * columns * share, transcendentals=0),
        name="split",
    )(place[None], proj_weight, spread)

    came = {}
    for n in range(len(sizes)):
        for k in range(1, POOL):
            came[n, k] = shift(pieces[1 + (k - 1) * len(sizes) + n], k)
    *late, _ = lax.optimization_barrier((*(came[0, k] for k in range(1, POOL)), parts[2 * groups + 2]))
    extras = [extra] + [x[sizes[0] :].reshape(extra.shape) for x in late]
    extra = lax.optimization_barrier(jnp.concatenate(extras, axis=0))
    parts += [extra] + [across(extra, flip) for flip in range(1, groups)]
    scalars = [*slots, *((group ^ flip) * depth for flip in range(groups))]
    hidden_all, counts_all, digits_all = pl.pallas_call(
        functools.partial(gather_kernel, groups, rows, depth, count_rows),
        out_shape=[
            jax.ShapeDtypeStruct((POOL, rows, groups * depth), hidden.dtype),
            jax.ShapeDtypeStruct((POOL, groups * count_rows, rows), jnp.bfloat16),
            jax.ShapeDtypeStruct((POOL, DIGIT_ROWS, rows), jnp.bfloat16),
        ],
        in_specs=[SMEM] + [HBM] * len(parts),
        out_specs=[VMEM] * 3,
        scratch_shapes=[pltpu.SemaphoreType.DMA((POOL * (2 * groups + 1),))],
        compiler_params=PARAMS,
        cost_estimate=pl.CostEstimate(flops=10**9, bytes_accessed=2 * POOL * rows * full, transcendentals=0),
        name="gather",
    )(jnp.stack([jnp.asarray(s, jnp.int32) for s in scalars]), *parts)

    def gather_inner(x):
        if inner == 1:
            return [(x, 0)]
        if inner == 2:
            other = lax.ppermute(x, "subset", [(a, a ^ 1) for a in range(subsets)])
            return [(x, member * share), (other, (1 - member) * share)]
        index = [[a * inner + b for b in range(inner)] for a in range(POOL)]
        return [(lax.all_gather(x, "subset", axis=1, tiled=True, axis_index_groups=index), 0)]

    own_parts = gather_inner(pieces[0])
    base = group * columns + place * width
    state, offset = None, 0
    for n, size in enumerate(sizes):
        block = inner * share
        w = [(x, place * block + at, True) for x, at in own_parts]
        for k in range(1, POOL):
            source = lax.rem(place - k + POOL, POOL)
            w += [(x, source * block + at, False) for x, at in gather_inner(came[n, k])]
        scalars = jnp.stack([jnp.asarray(s, jnp.int32) for s in [base] + [at for _, at, _ in w]])
        state = pl.pallas_call(
            functools.partial(score_kernel, size, offset, len(w), [s for _, _, s in w], n == 0),
            out_shape=jax.ShapeDtypeStruct((3 * POOL, rows), jnp.float32),
            in_specs=[SMEM, VMEM] + ([VMEM] if n else []) + [HBM] * len(w) + [VMEM],
            out_specs=VMEM,
            scratch_shapes=[pltpu.VMEM((size, full), proj_weight.dtype), pltpu.SemaphoreType.DMA((len(w),))],
            compiler_params=PARAMS,
            cost_estimate=pl.CostEstimate(
                flops=2 * POOL * rows * full * size, bytes_accessed=2 * full * size, transcendentals=POOL * rows * size
            ),
        )(scalars, digits_all, *([state] if n else []), *[x for x, _, _ in w], hidden_all)
        offset += size

    parts = [state] + [across(state, k) for k in range(1, groups)]
    merged = pl.pallas_call(
        merge_kernel, out_shape=jax.ShapeDtypeStruct((3 * POOL, rows), jnp.float32), name="merge"
    )(*parts)
    parts = [merged] + [shift(merged, k) for k in range(1, POOL)]
    loss, own, means = pl.pallas_call(
        functools.partial(loss_kernel, POOL, float(subsets * rows)),
        out_shape=[
            jax.ShapeDtypeStruct((1, rows), jnp.float32),
            jax.ShapeDtypeStruct((1, resamples), jnp.float32),
            jax.ShapeDtypeStruct((POOL, groups * count_rows), jnp.float32),
        ],
        in_specs=[SMEM] + [VMEM] * (POOL + 1),
        scratch_shapes=[pltpu.VMEM((POOL, rows), jnp.float32)],
        name="losses",
    )(place[None], *parts, counts_all)
    if inner == 1:
        values = [means]
    elif inner == 2:
        values = [means, lax.ppermute(means, "subset", [(a, a ^ 1) for a in range(subsets)])]
    else:
        index = [[a * inner + b for b in range(inner)] for a in range(POOL)]
        every = lax.all_gather(means, "subset", axis_index_groups=index)
        values = [every[n] for n in range(inner)]
    quantiles = pl.pallas_call(
        functools.partial(rank_kernel, resamples, count_rows),
        out_shape=jax.ShapeDtypeStruct((1, ranks.shape[0]), jnp.float32),
        scratch_shapes=[pltpu.VMEM((POOL * inner, 1, groups * count_rows), jnp.float32)],
        name="ranks",
    )(ranks[None], *values)
    return loss[0], own, quantiles[0]


def plain(hidden, proj_weight, targets, counts, ranks):
    features = lax.all_gather(hidden, "vocab", axis=1, tiled=True)
    columns = proj_weight.shape[1]
    whole_weight = lax.all_gather(proj_weight, "subset", axis=0, tiled=True)
    logits = jnp.dot(features, whole_weight, preferred_element_type=jnp.float32)
    local_top = jnp.max(logits, axis=1)
    local_sum = jnp.sum(jnp.exp(logits - local_top[:, None]), axis=1)
    offset = targets - lax.axis_index("vocab") * columns
    hit = lax.iota(jnp.int32, columns)[None, :] == offset[:, None]
    picked = jnp.sum(jnp.where(hit, logits, 0.0), axis=1)
    top = lax.pmax(local_top, "vocab")
    total, target_logit = lax.psum((local_sum * jnp.exp(local_top - top), picked), "vocab")
    loss = top + jnp.log(total) - target_logit
    total_rows = 1.0 * lax.axis_size("subset") * loss.shape[0]
    means = (
        jnp.einsum("cno,o->cn", counts.astype(jnp.float32), loss, precision=lax.Precision.HIGHEST) / total_rows
    )
    grouped = lax.all_gather(means, "vocab", axis=1, tiled=True)
    values = jnp.sort(lax.all_gather(grouped, "subset", axis=0, tiled=True).reshape(-1))
    chosen = lax.iota(jnp.int32, values.shape[0])[:, None] == ranks[None, :]
    return loss, means, jnp.sum(jnp.where(chosen, values[:, None], 0.0), axis=0)


def solution(mesh):
    subsets, groups = mesh.shape["subset"], mesh.shape["vocab"]

    def body(hidden, proj_weight, targets, counts, ranks):
        rows, depth = hidden.shape
        columns = proj_weight.shape[1]
        fits = (
            subsets % POOL == 0
            and groups == 4
            and rows == depth
            and rows % proj_weight.shape[0] == 0
            and rows % LANES == 0
            and columns % (16 * POOL) == 0
            and counts.shape[1] <= LANES // groups
        )
        if not fits:
            return plain(hidden, proj_weight, targets, counts, ranks)
        return pooled(subsets, groups, hidden, proj_weight, targets, counts, ranks)

    return jax.shard_map(
        body,
        mesh=mesh,
        in_specs=(
            P("subset", "vocab"),
            P("subset", "vocab"),
            P("subset"),
            P("subset", "vocab", None),
            P(),
        ),
        out_specs=(P("subset"), P("subset", "vocab"), P()),
        check_vma=False,
    )
```
